32 devices in a mesh: fsdp: 8 (over z, y), dp: 4 (over x, core).
Axes of the slice: x: 2, y: 2, z: 4, core: 2. Of those that a mesh axis runs over, the one named last changes fastest.
Arguments:
- tokens: bfloat16 [32, 128, 3584], P(('fsdp', 'dp')), may hold values from -6 to 6
- lengths: int32 [32], P(('fsdp', 'dp')), may hold values from 32 to 128
- partner: int32 [32], replicated, may hold values from 0 to 31, as said below
- pair_weight: float32 [32], P(('fsdp', 'dp')), may hold values from 0.25 to 27
- norm_gain: float32 [3584], replicated, may hold values from 0.5 to 1.5
- qkv_weight: bfloat16 [3584, 4608], P('fsdp'), may hold values from -0.09375 to 0.09375
- qkv_bias: float32 [4608], replicated, may hold values from -40 to 40
- out_weight: bfloat16 [3584, 3584], P(None, 'fsdp'), may hold values from -0.09375 to 0.09375
- final_gain: float32 [3584], replicated, may hold values from 0.5 to 1.5
- value_head: float32 [3584], replicated, may hold values from -0.09375 to 0.09375
Outputs:
- hidden: bfloat16 [32, 128, 3584], P(('fsdp', 'dp'))
- margins: float32 [32], P(('fsdp', 'dp'))
- loss: float32 [], replicated
The draws below stay inside these ranges and needn't reach their ends.
Inputs may be any that keep to these rules, and one draw needn't show every extreme that they name: partner[partner[i]] = i and partner[i] != i.
All inputs are finite; a program needn't handle non-finite values.
Results may differ from the reference program's by a relative error of at most 0.013.
The reference program's roundings to bfloat16 on the way count: a program that leaves them out, or rounds other values in their place, can miss the bound.
Values may be sent and summed in bfloat16 or wider, within the bound.
A program may use at most 128 MiB of HBM per device.

```python
import jax
import jax.numpy as jnp
from jax import lax

D = 3584
QUERY_HEADS = 28
KEY_VALUE_HEADS = 4
HEAD_SIZE = 128
SEQUENCE_TOKENS = 128
QUERY_FEATURES = 3584
KEY_FEATURES = 512
QKV = 4608
SEQS = 32


def draw_partner(key, part):
    half = SEQS // 2
    anchor = jax.random.randint(jax.random.fold_in(key, 31), (), 0, half - 2).astype(jnp.int32)
    ranks = jax.random.permutation(jax.random.fold_in(key, 32), SEQS).astype(jnp.int32)
    index = jnp.arange(SEQS, dtype=jnp.int32)
    far_end = anchor + half
    near_one = anchor + 1
    near_two = anchor + 2
    used = (index == anchor) | (index == far_end) | (index == near_one) | (index == near_two)
    sort_key = jnp.where(used, SEQS + ranks, ranks)
    order = jnp.argsort(sort_key, stable=True).astype(jnp.int32)
    rest = order[:SEQS - 4]
    first = rest[0::2]
    second = rest[1::2]
    result = jnp.zeros((SEQS,), jnp.int32)
    result = result.at[first].set(second)
    result = result.at[second].set(first)
    result = result.at[anchor].set(far_end)
    result = result.at[far_end].set(anchor)
    result = result.at[near_one].set(near_two)
    result = result.at[near_two].set(near_one)
    return result


def draw_pair_weight(key, part):
    position = jnp.arange(SEQS, dtype=jnp.float32) / jnp.float32(max(SEQS - 1, 1))
    rising = jnp.exp(position * jnp.log(jnp.float32(9.0)))
    rough = jax.random.uniform(jax.random.fold_in(key, 22), (SEQS,), jnp.float32, 0.5, 1.5)
    return jnp.clip(rising * rough, 0.25, 27.0).astype(jnp.float32)


def draw_qkv_bias(key, part):
    key_three = jax.random.fold_in(key, 13)
    result = 0.5 * jax.random.normal(key_three, (QKV,), jnp.float32)
    return jnp.clip(result, -40.0, 40.0).astype(jnp.float32)


def plant(entries, stream_key, smallest, top_value):
    place = [jax.random.randint(jax.random.fold_in(stream_key, axis), (), 0, length) for axis, length in enumerate(entries.shape)]
    main_axis = entries.shape.index(max(entries.shape))
    beside = place[:main_axis] + [(place[main_axis] + 1) % entries.shape[main_axis]] + place[main_axis + 1:]
    return entries.at[tuple(place)].set(smallest).at[tuple(beside)].set(top_value)


def level_of(rng, dims, shards, low, high):
    def one(dim, parts):
        steps = jax.random.uniform(jax.random.fold_in(jax.random.fold_in(rng, 6), dim), (parts,), jnp.float32, low / len(shards), high / len(shards))
        return jnp.repeat(jnp.exp(steps), dims[dim] // parts).reshape((-1,) + (1,) * (len(dims) - dim - 1))

    level = one(*shards[0])
    for cut in shards[1:]:
        level = level * one(*cut)
    return level


def bell_draw(key, dims, scale, limit, split=(), kind=jnp.bfloat16):
    values = jax.random.normal(key, dims, jnp.float32) * scale
    if len(split) > 0:
        values = level_of(key, dims, split, -0.22, 0.18) * values
    return jnp.clip(values, min=-limit, max=limit).astype(kind)


def setup_inputs(seed: int = 0) -> dict:
    streams_of = jax.random.split(jax.random.key(seed), 11)
    return {
        "tokens": bell_draw(streams_of[0], (SEQS, SEQUENCE_TOKENS, D), 1.0, 6.0, ((0, 32),)),
        "lengths": plant(jax.random.randint(streams_of[1], (SEQS,), SEQUENCE_TOKENS // 4, SEQUENCE_TOKENS + 1), jax.random.fold_in(streams_of[1], 1), SEQUENCE_TOKENS // 4, SEQUENCE_TOKENS).astype(jnp.int32),
        "partner": draw_partner(jax.random.fold_in(streams_of[10], 71), 0),
        "pair_weight": draw_pair_weight(jax.random.fold_in(streams_of[10], 71), 0),
        "norm_gain": jnp.clip(1.0 + 0.1 * jax.random.normal(streams_of[4], (D,), jnp.float32), 0.5, 1.5),
        "qkv_weight": bell_draw(streams_of[5], (D, QKV), D ** -0.5, 0.09375, ((0, 8),)),
        "qkv_bias": draw_qkv_bias(jax.random.fold_in(streams_of[10], 71), 0),
        "out_weight": bell_draw(streams_of[7], (QUERY_FEATURES, D), QUERY_FEATURES ** -0.5, 0.09375, ((1, 8),)),
        "final_gain": jnp.clip(1.0 + 0.1 * jax.random.normal(streams_of[8], (D,), jnp.float32), 0.5, 1.5),
        "value_head": bell_draw(streams_of[9], (D,), D ** -0.5, 0.09375, (), jnp.float32),
    }


def rms_scale(value_rows, gain):
    return value_rows * lax.rsqrt(lax.optimization_barrier(jnp.mean(value_rows * value_rows, axis=-1, keepdims=True)) + 1e-06) * gain

def apply_rotary(heads):
    half = HEAD_SIZE // 2
    positions = jnp.arange(SEQUENCE_TOKENS, dtype=jnp.float32)
    freqs = jnp.exp(-(2.0 * jnp.arange(half, dtype=jnp.float32) / HEAD_SIZE) * jnp.log(jnp.float32(1000000.0)))
    angles = positions[:, None] * freqs[None, :]
    cosine = jnp.cos(angles)
    sine = jnp.sin(angles)
    first = heads[..., :half]
    second = heads[..., half:]
    return jnp.concatenate([first * cosine - second * sine, second * cosine + first * sine], axis=-1)

def one_sequence(sequence, length, norm_gain, qkv_weight, qkv_bias, out_weight, final_gain, value_head):
    normed = rms_scale(sequence.astype(jnp.float32), norm_gain).astype(jnp.bfloat16)
    query_key_value = jnp.dot(normed, qkv_weight, preferred_element_type=jnp.float32) + qkv_bias
    query_rows = query_key_value[:, :QUERY_FEATURES].reshape(SEQUENCE_TOKENS, QUERY_HEADS, HEAD_SIZE).transpose(1, 0, 2)
    key_rows = query_key_value[:, QUERY_FEATURES:QUERY_FEATURES + KEY_FEATURES].reshape(SEQUENCE_TOKENS, KEY_VALUE_HEADS, HEAD_SIZE).transpose(1, 0, 2)
    value_rows = query_key_value[:, QUERY_FEATURES + KEY_FEATURES:].reshape(SEQUENCE_TOKENS, KEY_VALUE_HEADS, HEAD_SIZE).transpose(1, 0, 2).astype(jnp.bfloat16)
    query_rows = apply_rotary(query_rows).astype(jnp.bfloat16).reshape(KEY_VALUE_HEADS, QUERY_HEADS // KEY_VALUE_HEADS, SEQUENCE_TOKENS, HEAD_SIZE)
    key_rows = apply_rotary(key_rows).astype(jnp.bfloat16)
    scores = jnp.einsum('gqtd,gsd->gqts', query_rows.astype(jnp.float32), key_rows.astype(jnp.float32)) / jnp.sqrt(jnp.float32(HEAD_SIZE))
    rows = jnp.arange(SEQUENCE_TOKENS, dtype=jnp.int32)
    allowed = (rows[None, :] <= rows[:, None]) & (rows[None, :] < length)
    scores = jnp.where(allowed, scores, jnp.float32(-1e+30))
    top = lax.optimization_barrier(jnp.max(scores, axis=-1, keepdims=True))
    expd = jnp.exp(scores - top)
    probs = (expd / lax.optimization_barrier(jnp.sum(expd, axis=-1, keepdims=True))).astype(jnp.bfloat16)
    attn = jnp.einsum('gqts,gsd->gqtd', probs.astype(jnp.float32), value_rows.astype(jnp.float32))
    attn = attn.reshape(QUERY_HEADS, SEQUENCE_TOKENS, HEAD_SIZE).transpose(1, 0, 2).reshape(SEQUENCE_TOKENS, QUERY_FEATURES).astype(jnp.bfloat16)
    hidden = (sequence.astype(jnp.float32) + jnp.dot(attn, out_weight, preferred_element_type=jnp.float32)).astype(jnp.bfloat16)
    last = lax.dynamic_slice_in_dim(hidden, (length - 1).astype(jnp.int32), 1, 0)[0].astype(jnp.float32)
    score = jnp.sum(rms_scale(last, final_gain) * value_head)
    return (hidden, score)

def reference(tokens, lengths, partner, pair_weight, norm_gain, qkv_weight, qkv_bias, out_weight, final_gain, value_head):

    def step(item):
        return one_sequence(item[0], item[1], norm_gain, qkv_weight, qkv_bias, out_weight, final_gain, value_head)
    hidden, scores = lax.map(step, (tokens, lengths))
    other = scores[partner]
    index = jnp.arange(SEQS, dtype=jnp.int32)
    margins = jnp.where(index < partner, scores - other, other - scores)
    loss = jnp.sum(pair_weight * jax.nn.softplus(-margins)) / SEQS
    return (hidden, margins, loss)
```

```python
import functools

import jax
import jax.numpy as jnp
import numpy as np
from jax import lax
from jax.experimental import pallas as pl
from jax.experimental.pallas import tpu as pltpu
from jax.sharding import PartitionSpec as P

QUERY_HEADS = 28
KEY_VALUE_HEADS = 4
HEAD_SIZE = 128
QUERY_FEATURES = 3584
KEY_FEATURES = 512


def rms_scale(value_rows, gain):
    return (
        value_rows
        * lax.rsqrt(jnp.mean(value_rows * value_rows, axis=-1, keepdims=True) + 1e-06)
        * gain
    )


def apply_rotary(heads, length_rows):
    half = HEAD_SIZE // 2
    positions = jnp.arange(length_rows, dtype=jnp.float32)
    freqs = jnp.exp(
        -(2.0 * jnp.arange(half, dtype=jnp.float32) / HEAD_SIZE) * jnp.log(jnp.float32(1000000.0))
    )
    angles = positions[:, None] * freqs[None, :]
    cosine = jnp.cos(angles)
    sine = jnp.sin(angles)
    first = heads[..., :half]
    second = heads[..., half:]
    return jnp.concatenate(
        [first * cosine - second * sine, second * cosine + first * sine], axis=-1
    )


def attend(query_key_value, group_lengths, query_heads, key_value_heads):
    seq_count, length_rows, _ = query_key_value.shape
    query_width = query_heads * HEAD_SIZE
    key_width = key_value_heads * HEAD_SIZE
    query_rows = (
        query_key_value[..., :query_width]
        .reshape(seq_count, length_rows, query_heads, HEAD_SIZE)
        .transpose(0, 2, 1, 3)
    )
    key_rows = (
        query_key_value[..., query_width : query_width + key_width]
        .reshape(seq_count, length_rows, key_value_heads, HEAD_SIZE)
        .transpose(0, 2, 1, 3)
    )
    value_rows = (
        query_key_value[..., query_width + key_width :]
        .reshape(seq_count, length_rows, key_value_heads, HEAD_SIZE)
        .transpose(0, 2, 1, 3)
        .astype(jnp.bfloat16)
    )
    query_rows = (
        apply_rotary(query_rows, length_rows)
        .astype(jnp.bfloat16)
        .reshape(seq_count, key_value_heads, query_heads // key_value_heads, length_rows, HEAD_SIZE)
    )
    key_rows = apply_rotary(key_rows, length_rows).astype(jnp.bfloat16)
    scores = jnp.einsum(
        "bgqtd,bgsd->bgqts", query_rows, key_rows, preferred_element_type=jnp.float32
    ) / jnp.sqrt(jnp.float32(HEAD_SIZE))
    places = jnp.arange(length_rows, dtype=jnp.int32)
    causal = places[None, :] <= places[:, None]
    usable = places[None, :] < group_lengths[:, None]
    allowed = causal[None, :, :] & usable[:, None, :]
    scores = jnp.where(allowed[:, None, None, :, :], scores, jnp.float32(-1e30))
    highest = jnp.max(scores, axis=-1, keepdims=True)
    expd = jnp.exp(scores - highest)
    probs = (expd / jnp.sum(expd, axis=-1, keepdims=True)).astype(jnp.bfloat16)
    mixed = jnp.einsum("bgqts,bgsd->bgqtd", probs, value_rows, preferred_element_type=jnp.float32)
    mixed = mixed.reshape(seq_count, query_heads, length_rows, HEAD_SIZE).transpose(0, 2, 1, 3)
    return mixed.reshape(seq_count * length_rows, query_width).astype(jnp.bfloat16)


UP, DOWN, ACROSS = 0, 1, 2


def rotary_tables(length_rows):
    half = HEAD_SIZE // 2
    freqs = 1000000.0 ** (-2.0 * np.arange(half) / HEAD_SIZE)
    angles = np.arange(length_rows)[:, None] * freqs[None, :]
    cosine, sine = np.cos(angles), np.sin(angles)
    return (
        np.concatenate([cosine, cosine], axis=1).astype(np.float32),
        np.concatenate([-sine, sine], axis=1).astype(np.float32),
    )


def layer_kernel(
    shards,
    groups,
    tokens,
    qkv_weight,
    out_weight,
    lengths_tile,
    norm_gain,
    qkv_bias,
    cosine,
    sine,
    summed,
    qkv_full,
    out_full,
    tok_all,
    len_all,
    normed,
    qkv_rows,
    attn,
    own,
    part_out,
    part_in,
    local_sem,
    recv_sem,
    send_sem,
    tok_send,
    tok_recv,
    len_send,
    len_recv,
    part_send,
    part_recv,
):
    line = shards // 2
    f = lax.axis_index("fsdp")
    g = lax.axis_index("dp")
    z = f // 2
    y = f % 2
    even = z % 2 == 0
    seq_rows = tokens.shape[0]
    depth = qkv_weight.shape[0]
    width = tok_all.shape[2]
    query_cols = QUERY_FEATURES // groups
    key_cols = KEY_FEATURES // groups
    heads = query_cols // HEAD_SIZE
    half_depth = depth // 2
    half_out = query_cols // 2
    has_up = z < line - 1
    has_down = z > 0

    def slot(m, c, s):
        if m == 0:
            return qkv_full.at[pl.ds(pl.multiple_of(s * depth + c * half_depth, 32), half_depth)]
        return out_full.at[s, pl.ds(c * half_out, half_out)]

    locals_ = [[[], []], [[], []]]
    count = 0
    for c in range(2):
        rows = pl.ds(c * half_depth, half_depth)
        there = slot(0, c, f)
        for start, size, to in (
            (g * query_cols, query_cols, 0),
            (QUERY_FEATURES + g * key_cols, key_cols, query_cols),
            (QUERY_FEATURES + KEY_FEATURES + g * key_cols, key_cols, query_cols + key_cols),
        ):
            locals_[0][c].append(
                pltpu.make_async_copy(
                    qkv_weight.at[rows, pl.ds(pl.multiple_of(start, 128), size)],
                    there.at[:, pl.ds(to, size)],
                    local_sem.at[count],
                )
            )
            count += 1
    for c in range(2):
        locals_[1][c].append(
            pltpu.make_async_copy(
                out_weight.at[pl.ds(pl.multiple_of(g * query_cols + c * half_out, 32), half_out)],
                slot(1, c, f),
                local_sem.at[count],
            )
        )
        count += 1
    tok_local = pltpu.make_async_copy(tokens, tok_all.at[g], local_sem.at[count])
    len_local = pltpu.make_async_copy(lengths_tile, len_all.at[g], local_sem.at[count + 1])
    for m in range(2):
        for c in range(2):
            for copy in locals_[m][c]:
                copy.start()
    tok_local.start()
    len_local.start()

    barrier = pltpu.get_barrier_semaphore()
    across = 2 * z + 1 - y
    pl.semaphore_signal(barrier, inc=1, device_id={"fsdp": across})

    @pl.when(has_up)
    def _():
        pl.semaphore_signal(barrier, inc=1, device_id={"fsdp": f + 2})

    @pl.when(has_down)
    def _():
        pl.semaphore_signal(barrier, inc=1, device_id={"fsdp": f - 2})

    peers = [lax.rem(g + i, groups) for i in range(1, groups)]
    for peer in peers:
        pl.semaphore_signal(barrier, inc=1, device_id={"dp": peer})
    pl.semaphore_wait(barrier, groups + has_up.astype(jnp.int32) + has_down.astype(jnp.int32))

    started = []

    def send(cond, way, m, c, s):
        target = (f + 2, f - 2, across)[way]
        copy = pltpu.make_async_remote_copy(
            src_ref=slot(m, c, s),
            dst_ref=slot(m, c, s),
            send_sem=send_sem.at[way, m, c, s],
            recv_sem=recv_sem.at[m, c, s],
            device_id={"fsdp": target},
        )
        started.append((cond, copy))
        if cond is None:
            copy.start()
        else:
            pl.when(cond)(copy.start)

    def arrived(m, c, s):
        pltpu.make_async_copy(slot(m, c, s), slot(m, c, s), recv_sem.at[m, c, s]).wait()

    def own_line(m, c):
        send(has_up, UP, m, c, f)
        send(has_down, DOWN, m, c, f)

    def line_step(m, k):
        for c in range(2):
            below = z - k
            above = z + k
            s_below = 2 * jnp.maximum(below, 0) + y
            s_above = 2 * jnp.minimum(above, line - 1) + y

            @pl.when(below >= 0)
            def _():
                arrived(m, c, s_below)

            send((below >= 0) & has_up, UP, m, c, s_below)
            if k > 1 or c == 0:
                send(below >= 0, ACROSS, m, c, s_below)
            else:
                send((below >= 0) & even, ACROSS, m, c, s_below)

            @pl.when(above < line)
            def _():
                arrived(m, c, s_above)

            send((above < line) & has_down, DOWN, m, c, s_above)
            if k > 1 or c == 0:
                send(above < line, ACROSS, m, c, s_above)
            else:
                send((above < line) & jnp.logical_not(even), ACROSS, m, c, s_above)

    def half_step(m):
        arrived(m, 1, across)
        send(even, UP, m, 1, across)
        send(jnp.logical_not(even), DOWN, m, 1, across)

    for c in range(2):
        for copy in locals_[0][c]:
            copy.wait()
        own_line(0, c)
        send(None, ACROSS, 0, c, f)
    small = []
    for peer in peers:
        for source, dest, ss, rs in (
            (tokens, tok_all, tok_send, tok_recv),
            (lengths_tile, len_all, len_send, len_recv),
        ):
            copy = pltpu.make_async_remote_copy(
                src_ref=source,
                dst_ref=dest.at[g],
                send_sem=ss.at[peer],
                recv_sem=rs.at[g],
                device_id={"dp": peer},
            )
            copy.start()
            small.append(copy)

    line_step(0, 1)
    for k in range(2, line - 1):
        line_step(0, k)
    half_step(0)
    for c in range(2):
        for copy in locals_[1][c]:
            copy.wait()
        own_line(1, c)

    tok_local.wait()
    len_local.wait()
    for peer in peers:
        pltpu.make_async_copy(tok_all.at[peer], tok_all.at[peer], tok_recv.at[peer]).wait()
        pltpu.make_async_copy(len_all.at[peer], len_all.at[peer], len_recv.at[peer]).wait()

    norm_rows = 16
    for j in range(groups):

        @pl.loop(0, seq_rows // norm_rows)
        def _(i):
            at = pl.multiple_of(i * norm_rows, norm_rows)
            rows = tok_all[j, pl.ds(at, norm_rows), :].astype(jnp.float32)
            scale = lax.rsqrt(jnp.mean(rows * rows, axis=-1, keepdims=True) + 1e-06)
            normed[pl.ds(pl.multiple_of(j * seq_rows + at, norm_rows), norm_rows), :] = (
                rows * scale * norm_gain[...]
            ).astype(jnp.bfloat16)

    line_step(0, line - 1)
    for c in range(2):
        send(None, ACROSS, 1, c, f)

    def across_wait(m, k):
        for c in range(2):
            if k == 0:
                if c == 0:
                    arrived(m, c, across)
                continue
            for there, ok in ((z - k, z - k >= 0), (z + k, z + k < line)):
                s = 2 * jnp.clip(there, 0, line - 1) + 1 - y

                @pl.when(ok)
                def _():
                    arrived(m, c, s)

    for k in range(line):
        across_wait(0, k)

    tile = 3 * HEAD_SIZE

    @pl.loop(0, (query_cols + 2 * key_cols) // tile)
    def _(t):
        cols = pl.ds(pl.multiple_of(t * tile, tile), tile)
        qkv_rows[:, cols] = jnp.dot(
            normed[...], qkv_full[:, cols], preferred_element_type=jnp.float32
        )

    def head_rows(j, column, bias_at):
        rows = qkv_rows[pl.ds(pl.multiple_of(j * seq_rows, seq_rows), seq_rows), pl.ds(column, HEAD_SIZE)]
        return rows + qkv_bias[:, pl.ds(pl.multiple_of(bias_at, HEAD_SIZE), HEAD_SIZE)]

    def rotate(rows):
        return (
            rows * cosine[...] + pltpu.roll(rows, HEAD_SIZE // 2, 1) * sine[...]
        ).astype(jnp.bfloat16)

    key_heads = key_cols // HEAD_SIZE
    share = heads // key_heads

    def attend_sequence(j):
        query_place = lax.broadcasted_iota(jnp.int32, (seq_rows, seq_rows), 0)
        key_place = lax.broadcasted_iota(jnp.int32, (seq_rows, seq_rows), 1)
        allowed = (key_place <= query_place) & (key_place < len_all[j, 0:1, :])
        at = pl.ds(pl.multiple_of(j * seq_rows, seq_rows), seq_rows)
        for kh in range(key_heads):
            offset = kh * HEAD_SIZE
            key = rotate(
                head_rows(j, query_cols + offset, QUERY_FEATURES + g * key_cols + offset)
            )
            value = head_rows(
                j,
                query_cols + key_cols + offset,
                QUERY_FEATURES + KEY_FEATURES + g * key_cols + offset,
            ).astype(jnp.bfloat16)
            for h in range(kh * share, (kh + 1) * share):
                query = rotate(head_rows(j, h * HEAD_SIZE, g * query_cols + h * HEAD_SIZE))
                scores = lax.dot_general(
                    query, key, (((1,), (1,)), ((), ())), preferred_element_type=jnp.float32
                ) / np.float32(np.sqrt(HEAD_SIZE))
                scores = jnp.where(allowed, scores, jnp.float32(-1e30))
                expd = jnp.exp(scores - jnp.max(scores, axis=-1, keepdims=True))
                probs = (expd / jnp.sum(expd, axis=-1, keepdims=True)).astype(jnp.bfloat16)
                attn[at, h * HEAD_SIZE : (h + 1) * HEAD_SIZE] = jnp.dot(
                    probs, value, preferred_element_type=jnp.float32
                ).astype(jnp.bfloat16)

    pl.loop(0, groups // 2)(attend_sequence)
    line_step(1, 1)
    pl.loop(groups // 2, groups)(attend_sequence)

    def part_copy(peer, s):
        return pltpu.make_async_remote_copy(
            src_ref=part_out.at[s, pl.ds(pl.multiple_of(peer * seq_rows, seq_rows), seq_rows)],
            dst_ref=part_in.at[g, s],
            send_sem=part_send.at[peer, s],
            recv_sem=part_recv.at[g, s],
            device_id={"dp": peer},
        )

    def project(s):
        result = jnp.dot(attn[...], out_full[s], preferred_element_type=jnp.float32)
        part_out[s] = result.astype(jnp.bfloat16)
        for j in range(groups):

            @pl.when(g == j)
            def _():
                own[s] = result[j * seq_rows : (j + 1) * seq_rows]

        for peer in peers:
            part_copy(peer, s).start()

    def project_places(k, side):
        @pl.loop(0, 1 if k == 0 else 2)
        def _(i):
            there = z + (2 * i - 1) * k

            @pl.when((there >= 0) & (there < line))
            def _():
                project(2 * there + side)

    for k in range(2, line - 1):
        line_step(1, k)
    half_step(1)
    across_wait(1, 0)

    @pl.loop(0, 2)
    def _(side):
        project(2 * z + side)

    project_places(1, y)
    line_step(1, line - 1)
    for k in range(2, line):
        project_places(k, y)
    for k in range(1, line):
        across_wait(1, k)
        project_places(k, 1 - y)

    @pl.loop(0, shards)
    def _(s):
        total = own[s]
        for peer in peers:
            pltpu.make_async_copy(
                part_in.at[peer, s], part_in.at[peer, s], part_recv.at[peer, s]
            ).wait()
            total += part_in[peer, s].astype(jnp.float32)
        summed[s] = total

    for cond, copy in started:
        if cond is None:
            copy.wait_send()
        else:
            pl.when(cond)(copy.wait_send)
    for copy in small:
        copy.wait_send()

    @pl.loop(0, shards)
    def _(s):
        for peer in peers:
            part_copy(peer, s).wait_send()


def layer_fits(shards, groups, tokens, qkv_weight, out_weight):
    return (
        shards % 4 == 0
        and shards >= 8
        and qkv_weight.shape[0] % 32 == 0
        and KEY_VALUE_HEADS % groups == 0
        and tokens.shape[1] == HEAD_SIZE
        and groups % 2 == 0
    )


def layer(tokens, lengths, norm_gain, qkv_weight, qkv_bias, out_weight):
    shards, groups = lax.axis_size("fsdp"), lax.axis_size("dp")
    _, seq_rows, width = tokens.shape
    depth = qkv_weight.shape[0]
    out_cols = out_weight.shape[1]
    query_cols = QUERY_FEATURES // groups
    key_cols = KEY_FEATURES // groups
    all_cols = query_cols + 2 * key_cols
    rows = groups * seq_rows
    cosine, sine = rotary_tables(seq_rows)
    lengths_tile = jnp.broadcast_to(lengths[:, None], (8, seq_rows))
    dma = pltpu.SemaphoreType.DMA
    vmem = pl.BlockSpec(memory_space=pltpu.VMEM)
    anywhere = pl.BlockSpec(memory_space=pl.ANY)
    bf16, f32 = jnp.bfloat16, jnp.float32
    return pl.pallas_call(
        functools.partial(layer_kernel, shards, groups),
        out_shape=jax.ShapeDtypeStruct((shards, seq_rows, out_cols), f32),
        in_specs=[anywhere, anywhere, anywhere, vmem, vmem, vmem, vmem, vmem],
        out_specs=vmem,
        scratch_shapes=[
            pltpu.VMEM((shards * depth, all_cols), bf16),
            pltpu.VMEM((shards, query_cols, out_cols), bf16),
            pltpu.VMEM((groups, seq_rows, width), bf16),
            pltpu.VMEM((groups, 8, seq_rows), jnp.int32),
            pltpu.VMEM((rows, width), bf16),
            pltpu.VMEM((rows, all_cols), f32),
            pltpu.VMEM((rows, query_cols), bf16),
            pltpu.VMEM((shards, seq_rows, out_cols), f32),
            pltpu.VMEM((shards, rows, out_cols), bf16),
            pltpu.VMEM((groups, shards, seq_rows, out_cols), bf16),
            dma((10,)),
            dma((2, 2, shards)),
            dma((3, 2, 2, shards)),
            dma((groups,)),
            dma((groups,)),
            dma((groups,)),
            dma((groups,)),
            dma((groups, shards)),
            dma((groups, shards)),
        ],
        compiler_params=pltpu.CompilerParams(
            collective_id=0, has_side_effects=True, vmem_limit_bytes=60 * 1024 * 1024
        ),
    )(
        tokens[0],
        qkv_weight,
        out_weight,
        lengths_tile,
        norm_gain[None],
        qkv_bias[None],
        jnp.asarray(cosine),
        jnp.asarray(sine),
    )


def projected_by_gathers(
    tokens,
    lengths,
    norm_gain,
    qkv_weight,
    qkv_bias,
    out_weight,
):
    sequence = tokens[0]
    length_rows = sequence.shape[0]
    width = sequence.shape[1]
    normed = rms_scale(sequence.astype(jnp.float32), norm_gain).astype(jnp.bfloat16)
    query_group_count = lax.axis_size("dp")
    group_index = lax.axis_index("dp")
    query_heads = QUERY_HEADS // query_group_count
    key_value_heads = KEY_VALUE_HEADS // query_group_count
    query_cols = query_heads * HEAD_SIZE
    key_cols = key_value_heads * HEAD_SIZE
    group_normed, group_lengths = (
        lax.all_gather(normed[None], "dp", axis=0, tiled=True),
        lax.all_gather(lengths, "dp", axis=0, tiled=True),
    )
    seq_count = group_normed.shape[0]
    flat = group_normed.reshape(seq_count * length_rows, width)
    qkv_cols = jnp.concatenate(
        [
            lax.dynamic_slice_in_dim(qkv_weight, group_index * query_cols, query_cols, 1),
            lax.dynamic_slice_in_dim(
                qkv_weight, QUERY_FEATURES + group_index * key_cols, key_cols, 1
            ),
            lax.dynamic_slice_in_dim(
                qkv_weight, QUERY_FEATURES + KEY_FEATURES + group_index * key_cols, key_cols, 1
            ),
        ],
        axis=1,
    )
    bias_cols = jnp.concatenate(
        [
            lax.dynamic_slice_in_dim(qkv_bias, group_index * query_cols, query_cols, 0),
            lax.dynamic_slice_in_dim(
                qkv_bias, QUERY_FEATURES + group_index * key_cols, key_cols, 0
            ),
            lax.dynamic_slice_in_dim(
                qkv_bias, QUERY_FEATURES + KEY_FEATURES + group_index * key_cols, key_cols, 0
            ),
        ],
        axis=0,
    )
    out_rows = lax.dynamic_slice_in_dim(out_weight, group_index * query_cols, query_cols, 0)
    qkv_full, out_full = (
        lax.all_gather(qkv_cols, "fsdp", axis=0, tiled=True),
        lax.all_gather(out_rows, "fsdp", axis=1, tiled=True),
    )
    query_key_value = jnp.dot(flat, qkv_full, preferred_element_type=jnp.float32) + bias_cols
    attn = attend(
        query_key_value.reshape(seq_count, length_rows, -1),
        group_lengths,
        query_heads,
        key_value_heads,
    )
    return lax.psum_scatter(
        jnp.dot(attn, out_full, preferred_element_type=jnp.float32),
        "dp",
        scatter_dimension=0,
        tiled=True,
    )


def per_device(
    tokens,
    lengths,
    partner,
    pair_weight,
    norm_gain,
    qkv_weight,
    qkv_bias,
    out_weight,
    final_gain,
    value_head,
):
    sequence = tokens[0]
    length = lengths[0]
    args = (tokens, lengths, norm_gain, qkv_weight, qkv_bias, out_weight)
    if layer_fits(lax.axis_size("fsdp"), lax.axis_size("dp"), tokens, qkv_weight, out_weight):
        projected = layer(*args).transpose(1, 0, 2).reshape(sequence.shape)
    else:
        projected = projected_by_gathers(*args)
    hidden = (sequence.astype(jnp.float32) + projected).astype(jnp.bfloat16)
    last = lax.dynamic_slice_in_dim(hidden, length - 1, 1, 0)[0].astype(jnp.float32)
    score = jnp.sum(rms_scale(last, final_gain) * value_head)
    everyone, weights_all = (
        lax.all_gather(score.reshape(1), ("fsdp", "dp"), axis=0, tiled=True),
        lax.all_gather(pair_weight, ("fsdp", "dp"), axis=0, tiled=True),
    )
    total_seqs = everyone.shape[0]
    mine = lax.axis_index(("fsdp", "dp"))
    index_all = jnp.arange(total_seqs, dtype=jnp.int32)
    my_partner = jnp.sum(jnp.where(index_all == mine, partner, 0))
    other = jnp.sum(jnp.where(index_all == my_partner, everyone, jnp.float32(0.0)))
    margin = jnp.where(mine < my_partner, score - other, other - score)
    matches = partner[:, None] == index_all[None, :]
    others_all = jnp.sum(jnp.where(matches, everyone[None, :], jnp.float32(0.0)), axis=1)
    margins_all = jnp.where(index_all < partner, everyone - others_all, others_all - everyone)
    loss = jnp.sum(weights_all * jax.nn.softplus(-margins_all)) / total_seqs
    return (hidden[None], margin.reshape(1), loss)


def solution(mesh):
    return jax.shard_map(
        per_device,
        mesh=mesh,
        in_specs=(
            P(("fsdp", "dp"), None, None),
            P(("fsdp", "dp")),
            P(),
            P(("fsdp", "dp")),
            P(),
            P("fsdp", None),
            P(),
            P(None, "fsdp"),
            P(),
            P(),
        ),
        out_specs=(P(("fsdp", "dp"), None, None), P(("fsdp", "dp")), P()),
        check_vma=False,
    )
```

```python
import functools

import jax
import jax.numpy as jnp
import numpy as np
from jax import lax
from jax.experimental import pallas as pl
from jax.experimental.pallas import tpu as pltpu
from jax.sharding import PartitionSpec as P

QUERY_HEADS = 28
KEY_VALUE_HEADS = 4
HEAD_SIZE = 128
QUERY_FEATURES = 3584
KEY_FEATURES = 512


def rms_scale(value_rows, gain):
    return (
        value_rows
        * lax.rsqrt(jnp.mean(value_rows * value_rows, axis=-1, keepdims=True) + 1e-06)
        * gain
    )


def apply_rotary(heads, length_rows):
    half = HEAD_SIZE // 2
    positions = jnp.arange(length_rows, dtype=jnp.float32)
    freqs = jnp.exp(
        -(2.0 * jnp.arange(half, dtype=jnp.float32) / HEAD_SIZE) * jnp.log(jnp.float32(1000000.0))
    )
    angles = positions[:, None] * freqs[None, :]
    cosine = jnp.cos(angles)
    sine = jnp.sin(angles)
    first = heads[..., :half]
    second = heads[..., half:]
    return jnp.concatenate(
        [first * cosine - second * sine, second * cosine + first * sine], axis=-1
    )


def attend(query_key_value, group_lengths, query_heads, key_value_heads):
    seq_count, length_rows, _ = query_key_value.shape
    query_width = query_heads * HEAD_SIZE
    key_width = key_value_heads * HEAD_SIZE
    query_rows = (
        query_key_value[..., :query_width]
        .reshape(seq_count, length_rows, query_heads, HEAD_SIZE)
        .transpose(0, 2, 1, 3)
    )
    key_rows = (
        query_key_value[..., query_width : query_width + key_width]
        .reshape(seq_count, length_rows, key_value_heads, HEAD_SIZE)
        .transpose(0, 2, 1, 3)
    )
    value_rows = (
        query_key_value[..., query_width + key_width :]
        .reshape(seq_count, length_rows, key_value_heads, HEAD_SIZE)
        .transpose(0, 2, 1, 3)
        .astype(jnp.bfloat16)
    )
    query_rows = (
        apply_rotary(query_rows, length_rows)
        .astype(jnp.bfloat16)
        .reshape(seq_count, key_value_heads, query_heads // key_value_heads, length_rows, HEAD_SIZE)
    )
    key_rows = apply_rotary(key_rows, length_rows).astype(jnp.bfloat16)
    scores = jnp.einsum(
        "bgqtd,bgsd->bgqts", query_rows, key_rows, preferred_element_type=jnp.float32
    ) / jnp.sqrt(jnp.float32(HEAD_SIZE))
    places = jnp.arange(length_rows, dtype=jnp.int32)
    causal = places[None, :] <= places[:, None]
    usable = places[None, :] < group_lengths[:, None]
    allowed = causal[None, :, :] & usable[:, None, :]
    scores = jnp.where(allowed[:, None, None, :, :], scores, jnp.float32(-1e30))
    highest = jnp.max(scores, axis=-1, keepdims=True)
    expd = jnp.exp(scores - highest)
    probs = (expd / jnp.sum(expd, axis=-1, keepdims=True)).astype(jnp.bfloat16)
    mixed = jnp.einsum("bgqts,bgsd->bgqtd", probs, value_rows, preferred_element_type=jnp.float32)
    mixed = mixed.reshape(seq_count, query_heads, length_rows, HEAD_SIZE).transpose(0, 2, 1, 3)
    return mixed.reshape(seq_count * length_rows, query_width).astype(jnp.bfloat16)


UP, DOWN, ACROSS = 0, 1, 2


def rotary_tables(length_rows):
    half = HEAD_SIZE // 2
    freqs = 1000000.0 ** (-2.0 * np.arange(half) / HEAD_SIZE)
    angles = np.arange(length_rows)[:, None] * freqs[None, :]
    cosine, sine = np.cos(angles), np.sin(angles)
    return (
        np.concatenate([cosine, cosine], axis=1).astype(np.float32),
        np.concatenate([-sine, sine], axis=1).astype(np.float32),
    )


def layer_kernel(
    shards,
    groups,
    tokens,
    qkv_weight,
    out_weight,
    length,
    pair_weight,
    partner,
    norm_gain,
    final_gain,
    value_head,
    qkv_bias,
    cosine,
    sine,
    hidden,
    margin_out,
    loss_out,
    qkv_full,
    out_full,
    tok_all,
    len_tile,
    len_all,
    normed,
    qkv_rows,
    attn,
    own,
    part_out,
    part_in,
    score_tile,
    score_all,
    partner_rows,
    local_sem,
    recv_sem,
    send_sem,
    tok_send,
    tok_recv,
    len_send,
    len_recv,
    part_send,
    part_recv,
    score_send,
    score_recv,
):
    line = shards // 2
    f = lax.axis_index("fsdp")
    g = lax.axis_index("dp")
    z = f // 2
    y = f % 2
    even = z % 2 == 0
    seq_rows = tokens.shape[0]
    depth = qkv_weight.shape[0]
    width = tok_all.shape[2]
    query_cols = QUERY_FEATURES // groups
    key_cols = KEY_FEATURES // groups
    heads = query_cols // HEAD_SIZE
    half_depth = depth // 2
    half_out = out_weight.shape[0] // 2
    has_up = z < line - 1
    has_down = z > 0

    def slot(m, c, s):
        if m == 0:
            return qkv_full.at[pl.ds(pl.multiple_of(s * depth + c * half_depth, 32), half_depth)]
        return out_full.at[s, pl.ds(c * half_out, half_out)]

    locals_ = [[[], []], [[], []]]
    count = 0
    for c in range(2):
        rows = pl.ds(c * half_depth, half_depth)
        there = slot(0, c, f)
        for start, size, to in (
            (g * query_cols, query_cols, 0),
            (QUERY_FEATURES + g * key_cols, key_cols, query_cols),
            (QUERY_FEATURES + KEY_FEATURES + g * key_cols, key_cols, query_cols + key_cols),
        ):
            locals_[0][c].append(
                pltpu.make_async_copy(
                    qkv_weight.at[rows, pl.ds(pl.multiple_of(start, 128), size)],
                    there.at[:, pl.ds(to, size)],
                    local_sem.at[count],
                )
            )
            count += 1
    for c in range(2):
        locals_[1][c].append(
            pltpu.make_async_copy(
                out_weight.at[
                    pl.ds(c * half_out, half_out),
                    pl.ds(pl.multiple_of(g * query_cols, 128), query_cols),
                ],
                slot(1, c, f),
                local_sem.at[count],
            )
        )
        count += 1
    tok_local = pltpu.make_async_copy(tokens, tok_all.at[g], local_sem.at[count])
    len_tile[...] = jnp.full(len_tile.shape, length[0], jnp.int32)
    len_all[g] = len_tile[...]
    for m in range(2):
        for c in range(2):
            for copy in locals_[m][c]:
                copy.start()
    tok_local.start()

    barrier = pltpu.get_barrier_semaphore()
    across = 2 * z + 1 - y
    everyone = shards * groups
    me = f * groups + g

    @pl.loop(1, everyone)
    def _(i):
        other = lax.rem(me + i, everyone)
        pl.semaphore_signal(
            barrier, inc=1, device_id={"fsdp": other // groups, "dp": lax.rem(other, groups)}
        )

    peers = [lax.rem(g + i, groups) for i in range(1, groups)]
    pl.semaphore_wait(barrier, everyone - 1)

    started = []

    def send(cond, way, m, c, s):
        target = (f + 2, f - 2, across)[way]
        copy = pltpu.make_async_remote_copy(
            src_ref=slot(m, c, s),
            dst_ref=slot(m, c, s),
            send_sem=send_sem.at[way, m, c, s],
            recv_sem=recv_sem.at[m, c, s],
            device_id={"fsdp": target},
        )
        started.append((cond, copy))
        if cond is None:
            copy.start()
        else:
            pl.when(cond)(copy.start)

    def arrived(m, c, s):
        pltpu.make_async_copy(slot(m, c, s), slot(m, c, s), recv_sem.at[m, c, s]).wait()

    def own_line(m, c):
        send(has_up, UP, m, c, f)
        send(has_down, DOWN, m, c, f)

    def line_step(m, k):
        for c in range(2):
            below = z - k
            above = z + k
            s_below = 2 * jnp.maximum(below, 0) + y
            s_above = 2 * jnp.minimum(above, line - 1) + y

            @pl.when(below >= 0)
            def _():
                arrived(m, c, s_below)

            send((below >= 0) & has_up, UP, m, c, s_below)
            if k > 1 or c == 0:
                send(below >= 0, ACROSS, m, c, s_below)
            else:
                send((below >= 0) & even, ACROSS, m, c, s_below)

            @pl.when(above < line)
            def _():
                arrived(m, c, s_above)

            send((above < line) & has_down, DOWN, m, c, s_above)
            if k > 1 or c == 0:
                send(above < line, ACROSS, m, c, s_above)
            else:
                send((above < line) & jnp.logical_not(even), ACROSS, m, c, s_above)

    def half_step(m):
        arrived(m, 1, across)
        send(even, UP, m, 1, across)
        send(jnp.logical_not(even), DOWN, m, 1, across)

    for c in range(2):
        for copy in locals_[0][c]:
            copy.wait()
        own_line(0, c)
        send(None, ACROSS, 0, c, f)
    small = []
    for peer in peers:
        for source, dest, ss, rs in (
            (tokens, tok_all, tok_send, tok_recv),
            (len_tile, len_all, len_send, len_recv),
        ):
            copy = pltpu.make_async_remote_copy(
                src_ref=source,
                dst_ref=dest.at[g],
                send_sem=ss.at[peer],
                recv_sem=rs.at[g],
                device_id={"dp": peer},
            )
            copy.start()
            small.append(copy)

    line_step(0, 1)
    for k in range(2, line - 1):
        line_step(0, k)
    half_step(0)
    for c in range(2):
        for copy in locals_[1][c]:
            copy.wait()
        own_line(1, c)

    tok_local.wait()
    for peer in peers:
        pltpu.make_async_copy(tok_all.at[peer], tok_all.at[peer], tok_recv.at[peer]).wait()
        pltpu.make_async_copy(len_all.at[peer], len_all.at[peer], len_recv.at[peer]).wait()

    norm_rows = 16
    for j in range(groups):

        @pl.loop(0, seq_rows // norm_rows)
        def _(i):
            at = pl.multiple_of(i * norm_rows, norm_rows)
            rows = tok_all[j, pl.ds(at, norm_rows), :].astype(jnp.float32)
            scale = lax.rsqrt(jnp.mean(rows * rows, axis=-1, keepdims=True) + 1e-06)
            normed[pl.ds(pl.multiple_of(j * seq_rows + at, norm_rows), norm_rows), :] = (
                rows * scale * norm_gain[...]
            ).astype(jnp.bfloat16)

    line_step(0, line - 1)
    for c in range(2):
        send(None, ACROSS, 1, c, f)

    def across_wait(m, k):
        for c in range(2):
            if k == 0:
                if c == 0:
                    arrived(m, c, across)
                continue
            for there, ok in ((z - k, z - k >= 0), (z + k, z + k < line)):
                s = 2 * jnp.clip(there, 0, line - 1) + 1 - y

                @pl.when(ok)
                def _():
                    arrived(m, c, s)

    for k in range(line):
        across_wait(0, k)

    tile = 3 * HEAD_SIZE

    @pl.loop(0, (query_cols + 2 * key_cols) // tile)
    def _(t):
        cols = pl.ds(pl.multiple_of(t * tile, tile), tile)
        qkv_rows[:, cols] = jnp.dot(
            normed[...], qkv_full[:, cols], preferred_element_type=jnp.float32
        )

    def head_rows(j, column, bias_at):
        rows = qkv_rows[pl.ds(pl.multiple_of(j * seq_rows, seq_rows), seq_rows), pl.ds(column, HEAD_SIZE)]
        return rows + qkv_bias[:, pl.ds(pl.multiple_of(bias_at, HEAD_SIZE), HEAD_SIZE)]

    def rotate(rows):
        return (
            rows * cosine[...] + pltpu.roll(rows, HEAD_SIZE // 2, 1) * sine[...]
        ).astype(jnp.bfloat16)

    key_heads = key_cols // HEAD_SIZE
    share = heads // key_heads

    def attend_sequence(j):
        query_place = lax.broadcasted_iota(jnp.int32, (seq_rows, seq_rows), 0)
        key_place = lax.broadcasted_iota(jnp.int32, (seq_rows, seq_rows), 1)
        allowed = (key_place <= query_place) & (key_place < len_all[j, 0:1, :])
        at = pl.ds(pl.multiple_of(j * seq_rows, seq_rows), seq_rows)
        for kh in range(key_heads):
            offset = kh * HEAD_SIZE
            key = rotate(
                head_rows(j, query_cols + offset, QUERY_FEATURES + g * key_cols + offset)
            )
            value = head_rows(
                j,
                query_cols + key_cols + offset,
                QUERY_FEATURES + KEY_FEATURES + g * key_cols + offset,
            ).astype(jnp.bfloat16)
            for h in range(kh * share, (kh + 1) * share):
                query = rotate(head_rows(j, h * HEAD_SIZE, g * query_cols + h * HEAD_SIZE))
                scores = lax.dot_general(
                    query, key, (((1,), (1,)), ((), ())), preferred_element_type=jnp.float32
                ) / np.float32(np.sqrt(HEAD_SIZE))
                scores = jnp.where(allowed, scores, jnp.float32(-1e30))
                expd = jnp.exp(scores - jnp.max(scores, axis=-1, keepdims=True))
                probs = (expd / jnp.sum(expd, axis=-1, keepdims=True)).astype(jnp.bfloat16)
                attn[at, h * HEAD_SIZE : (h + 1) * HEAD_SIZE] = jnp.dot(
                    probs, value, preferred_element_type=jnp.float32
                ).astype(jnp.bfloat16)

    pl.loop(0, groups // 2)(attend_sequence)
    line_step(1, 1)
    pl.loop(groups // 2, groups)(attend_sequence)

    def part_copy(peer, s):
        return pltpu.make_async_remote_copy(
            src_ref=part_out.at[s, pl.ds(pl.multiple_of(peer * seq_rows, seq_rows), seq_rows)],
            dst_ref=part_in.at[g, s],
            send_sem=part_send.at[peer, s],
            recv_sem=part_recv.at[g, s],
            device_id={"dp": peer},
        )

    def project(s):
        result = lax.dot_general(
            attn[...],
            out_full[s],
            (((1,), (1,)), ((), ())),
            preferred_element_type=jnp.float32,
        )
        part_out[s] = result.astype(jnp.bfloat16)
        for j in range(groups):

            @pl.when(g == j)
            def _():
                own[s] = result[j * seq_rows : (j + 1) * seq_rows]

        for peer in peers:
            part_copy(peer, s).start()

    def project_places(k, side):
        @pl.loop(0, 1 if k == 0 else 2)
        def _(i):
            there = z + (2 * i - 1) * k

            @pl.when((there >= 0) & (there < line))
            def _():
                project(2 * there + side)

    for k in range(2, line - 1):
        line_step(1, k)
    half_step(1)
    across_wait(1, 0)

    @pl.loop(0, 2)
    def _(side):
        project(2 * z + side)

    project_places(1, y)
    line_step(1, line - 1)
    for k in range(2, line):
        project_places(k, y)
    for k in range(1, line):
        across_wait(1, k)
        project_places(k, 1 - y)

    @pl.loop(0, shards)
    def _(s):
        for peer in peers:
            pltpu.make_async_copy(
                part_in.at[peer, s], part_in.at[peer, s], part_recv.at[peer, s]
            ).wait()

    block = 32
    out_cols = own.shape[2]

    @pl.loop(0, seq_rows // block)
    def _(i):
        at = pl.ds(pl.multiple_of(i * block, block), block)
        for p in range(shards // 2):
            sums = []
            for s in (2 * p, 2 * p + 1):
                total = own[s, at]
                for peer in peers:
                    total += part_in[peer, s, at].astype(jnp.float32)
                sums.append(total)
            cols = slice(2 * p * out_cols, 2 * (p + 1) * out_cols)
            hidden[at, cols] = (
                tok_all[g, at, cols].astype(jnp.float32) + jnp.concatenate(sums, axis=1)
            ).astype(jnp.bfloat16)

    place = lax.broadcasted_iota(jnp.int32, len_tile.shape, 1)
    pick = (place == len_tile[...] - 1).astype(jnp.bfloat16)
    last = jnp.dot(pick, hidden[...], preferred_element_type=jnp.float32)
    scale = lax.rsqrt(jnp.mean(last * last, axis=-1, keepdims=True) + 1e-06)
    score = jnp.sum(last * scale * final_gain[...] * value_head[...], axis=-1, keepdims=True)
    first_row = lax.broadcasted_iota(jnp.int32, score_tile.shape, 0) == 0
    score_tile[...] = jnp.where(first_row, score, jnp.full(score_tile.shape, pair_weight[0]))
    score_all[me] = score_tile[...]

    def score_copy(i):
        other = lax.rem(me + i, everyone)
        return pltpu.make_async_remote_copy(
            src_ref=score_tile,
            dst_ref=score_all.at[me],
            send_sem=score_send.at[other],
            recv_sem=score_recv.at[me],
            device_id={"fsdp": other // groups, "dp": lax.rem(other, groups)},
        )

    @pl.loop(1, everyone)
    def _(i):
        score_copy(i).start()

    @pl.loop(0, everyone)
    def _(i):
        partner_rows[pl.ds(i, 1), :] = jnp.full((1, HEAD_SIZE), partner[i], jnp.int32)

    @pl.loop(1, everyone)
    def _(i):
        other = lax.rem(me + i, everyone)
        pltpu.make_async_copy(
            score_all.at[other], score_all.at[other], score_recv.at[other]
        ).wait()

    scores = score_all[:, 0, :]
    weights = score_all[:, 1, :]
    row = lax.broadcasted_iota(jnp.int32, scores.shape, 0)
    lane = lax.broadcasted_iota(jnp.int32, scores.shape, 1)
    partners = partner_rows[...]
    score_row = jnp.sum(jnp.where(row == lane, scores, 0.0), axis=0, keepdims=True)
    others = jnp.sum(jnp.where(partners == lane, score_row, 0.0), axis=1, keepdims=True)
    margins = jnp.where(row < partners, scores - others, others - scores)
    softplus = jnp.maximum(-margins, 0.0) + jnp.log1p(jnp.exp(-jnp.abs(margins)))
    first_lane = lane == 0
    margin_out[0] = jnp.sum(jnp.where(first_lane & (row == me), margins, 0.0))
    loss_out[0] = jnp.sum(jnp.where(first_lane, weights * softplus, 0.0)) / everyone

    for cond, copy in started:
        if cond is None:
            copy.wait_send()
        else:
            pl.when(cond)(copy.wait_send)
    for copy in small:
        copy.wait_send()

    @pl.loop(0, shards)
    def _(s):
        for peer in peers:
            part_copy(peer, s).wait_send()

    @pl.loop(1, everyone)
    def _(i):
        score_copy(i).wait_send()


def layer_fits(shards, groups, tokens, qkv_weight, out_weight):
    return (
        shards % 4 == 0
        and shards >= 8
        and qkv_weight.shape[0] % 32 == 0
        and KEY_VALUE_HEADS % groups == 0
        and tokens.shape[1] == HEAD_SIZE
        and groups % 2 == 0
        and shards * groups <= HEAD_SIZE
        and out_weight.shape[1] % 64 == 0
    )


def layer(
    tokens,
    lengths,
    partner,
    pair_weight,
    norm_gain,
    qkv_weight,
    qkv_bias,
    out_weight,
    final_gain,
    value_head,
):
    shards, groups = lax.axis_size("fsdp"), lax.axis_size("dp")
    _, seq_rows, width = tokens.shape
    depth = qkv_weight.shape[0]
    out_cols = out_weight.shape[1]
    query_cols = QUERY_FEATURES // groups
    key_cols = KEY_FEATURES // groups
    all_cols = query_cols + 2 * key_cols
    rows = groups * seq_rows
    cosine, sine = rotary_tables(seq_rows)
    everyone = shards * groups
    dma = pltpu.SemaphoreType.DMA
    vmem = pl.BlockSpec(memory_space=pltpu.VMEM)
    anywhere = pl.BlockSpec(memory_space=pl.ANY)
    bf16, f32 = jnp.bfloat16, jnp.float32
    scalar = pl.BlockSpec(memory_space=pltpu.SMEM)
    hidden, margin, loss = pl.pallas_call(
        functools.partial(layer_kernel, shards, groups),
        out_shape=(
            jax.ShapeDtypeStruct((seq_rows, width), bf16),
            jax.ShapeDtypeStruct((1,), f32),
            jax.ShapeDtypeStruct((1,), f32),
        ),
        in_specs=[anywhere] * 3 + [scalar] * 3 + [vmem] * 6,
        out_specs=(vmem, scalar, scalar),
        scratch_shapes=[
            pltpu.VMEM((shards * depth, all_cols), bf16),
            pltpu.VMEM((shards, out_cols, query_cols), bf16),
            pltpu.VMEM((groups, seq_rows, width), bf16),
            pltpu.VMEM((8, seq_rows), jnp.int32),
            pltpu.VMEM((groups, 8, seq_rows), jnp.int32),
            pltpu.VMEM((rows, width), bf16),
            pltpu.VMEM((rows, all_cols), f32),
            pltpu.VMEM((rows, query_cols), bf16),
            pltpu.VMEM((shards, seq_rows, out_cols), f32),
            pltpu.VMEM((shards, rows, out_cols), bf16),
            pltpu.VMEM((groups, shards, seq_rows, out_cols), bf16),
            pltpu.VMEM((8, HEAD_SIZE), f32),
            pltpu.VMEM((everyone, 8, HEAD_SIZE), f32),
            pltpu.VMEM((everyone, HEAD_SIZE), jnp.int32),
            dma((10,)),
            dma((2, 2, shards)),
            dma((3, 2, 2, shards)),
            dma((groups,)),
            dma((groups,)),
            dma((groups,)),
            dma((groups,)),
            dma((groups, shards)),
            dma((groups, shards)),
            dma((everyone,)),
            dma((everyone,)),
        ],
        compiler_params=pltpu.CompilerParams(
            collective_id=0, has_side_effects=True, vmem_limit_bytes=60 * 1024 * 1024
        ),
    )(
        tokens[0],
        qkv_weight,
        out_weight.T,
        lengths,
        pair_weight,
        partner,
        norm_gain[None],
        final_gain[None],
        value_head[None],
        qkv_bias[None],
        jnp.asarray(cosine),
        jnp.asarray(sine),
    )
    return hidden[None], margin, loss.reshape(())


def projected_by_gathers(
    tokens,
    lengths,
    norm_gain,
    qkv_weight,
    qkv_bias,
    out_weight,
):
    sequence = tokens[0]
    length_rows = sequence.shape[0]
    width = sequence.shape[1]
    normed = rms_scale(sequence.astype(jnp.float32), norm_gain).astype(jnp.bfloat16)
    query_group_count = lax.axis_size("dp")
    group_index = lax.axis_index("dp")
    query_heads = QUERY_HEADS // query_group_count
    key_value_heads = KEY_VALUE_HEADS // query_group_count
    query_cols = query_heads * HEAD_SIZE
    key_cols = key_value_heads * HEAD_SIZE
    group_normed, group_lengths = (
        lax.all_gather(normed[None], "dp", axis=0, tiled=True),
        lax.all_gather(lengths, "dp", axis=0, tiled=True),
    )
    seq_count = group_normed.shape[0]
    flat = group_normed.reshape(seq_count * length_rows, width)
    qkv_cols = jnp.concatenate(
        [
            lax.dynamic_slice_in_dim(qkv_weight, group_index * query_cols, query_cols, 1),
            lax.dynamic_slice_in_dim(
                qkv_weight, QUERY_FEATURES + group_index * key_cols, key_cols, 1
            ),
            lax.dynamic_slice_in_dim(
                qkv_weight, QUERY_FEATURES + KEY_FEATURES + group_index * key_cols, key_cols, 1
            ),
        ],
        axis=1,
    )
    bias_cols = jnp.concatenate(
        [
            lax.dynamic_slice_in_dim(qkv_bias, group_index * query_cols, query_cols, 0),
            lax.dynamic_slice_in_dim(
                qkv_bias, QUERY_FEATURES + group_index * key_cols, key_cols, 0
            ),
            lax.dynamic_slice_in_dim(
                qkv_bias, QUERY_FEATURES + KEY_FEATURES + group_index * key_cols, key_cols, 0
            ),
        ],
        axis=0,
    )
    out_rows = lax.dynamic_slice_in_dim(out_weight, group_index * query_cols, query_cols, 0)
    qkv_full, out_full = (
        lax.all_gather(qkv_cols, "fsdp", axis=0, tiled=True),
        lax.all_gather(out_rows, "fsdp", axis=1, tiled=True),
    )
    query_key_value = jnp.dot(flat, qkv_full, preferred_element_type=jnp.float32) + bias_cols
    attn = attend(
        query_key_value.reshape(seq_count, length_rows, -1),
        group_lengths,
        query_heads,
        key_value_heads,
    )
    return lax.psum_scatter(
        jnp.dot(attn, out_full, preferred_element_type=jnp.float32),
        "dp",
        scatter_dimension=0,
        tiled=True,
    )


def per_device(
    tokens,
    lengths,
    partner,
    pair_weight,
    norm_gain,
    qkv_weight,
    qkv_bias,
    out_weight,
    final_gain,
    value_head,
):
    if layer_fits(lax.axis_size("fsdp"), lax.axis_size("dp"), tokens, qkv_weight, out_weight):
        return layer(
            tokens,
            lengths,
            partner,
            pair_weight,
            norm_gain,
            qkv_weight,
            qkv_bias,
            out_weight,
            final_gain,
            value_head,
        )
    sequence = tokens[0]
    length = lengths[0]
    projected = projected_by_gathers(tokens, lengths, norm_gain, qkv_weight, qkv_bias, out_weight)
    hidden = (sequence.astype(jnp.float32) + projected).astype(jnp.bfloat16)
    last = lax.dynamic_slice_in_dim(hidden, length - 1, 1, 0)[0].astype(jnp.float32)
    score = jnp.sum(rms_scale(last, final_gain) * value_head)
    everyone, weights_all = (
        lax.all_gather(score.reshape(1), ("fsdp", "dp"), axis=0, tiled=True),
        lax.all_gather(pair_weight, ("fsdp", "dp"), axis=0, tiled=True),
    )
    total_seqs = everyone.shape[0]
    mine = lax.axis_index(("fsdp", "dp"))
    index_all = jnp.arange(total_seqs, dtype=jnp.int32)
    my_partner = jnp.sum(jnp.where(index_all == mine, partner, 0))
    other = jnp.sum(jnp.where(index_all == my_partner, everyone, jnp.float32(0.0)))
    margin = jnp.where(mine < my_partner, score - other, other - score)
    matches = partner[:, None] == index_all[None, :]
    others_all = jnp.sum(jnp.where(matches, everyone[None, :], jnp.float32(0.0)), axis=1)
    margins_all = jnp.where(index_all < partner, everyone - others_all, others_all - everyone)
    loss = jnp.sum(weights_all * jax.nn.softplus(-margins_all)) / total_seqs
    return (hidden[None], margin.reshape(1), loss)


def solution(mesh):
    return jax.shard_map(
        per_device,
        mesh=mesh,
        in_specs=(
            P(("fsdp", "dp"), None, None),
            P(("fsdp", "dp")),
            P(),
            P(("fsdp", "dp")),
            P(),
            P("fsdp", None),
            P(),
            P(None, "fsdp"),
            P(),
            P(),
        ),
        out_specs=(P(("fsdp", "dp"), None, None), P(("fsdp", "dp")), P()),
        check_vma=False,
    )
```

```python
import functools

import jax
import jax.numpy as jnp
import numpy as np
from jax import lax
from jax.experimental import pallas as pl
from jax.experimental.pallas import tpu as pltpu
from jax.sharding import PartitionSpec as P

QUERY_HEADS = 28
KEY_VALUE_HEADS = 4
HEAD_SIZE = 128
QUERY_FEATURES = 3584
KEY_FEATURES = 512


def rms_scale(value_rows, gain):
    return (
        value_rows
        * lax.rsqrt(jnp.mean(value_rows * value_rows, axis=-1, keepdims=True) + 1e-06)
        * gain
    )


def apply_rotary(heads, length_rows):
    half = HEAD_SIZE // 2
    positions = jnp.arange(length_rows, dtype=jnp.float32)
    freqs = jnp.exp(
        -(2.0 * jnp.arange(half, dtype=jnp.float32) / HEAD_SIZE) * jnp.log(jnp.float32(1000000.0))
    )
    angles = positions[:, None] * freqs[None, :]
    cosine = jnp.cos(angles)
    sine = jnp.sin(angles)
    first = heads[..., :half]
    second = heads[..., half:]
    return jnp.concatenate(
        [first * cosine - second * sine, second * cosine + first * sine], axis=-1
    )


def attend(query_key_value, group_lengths, query_heads, key_value_heads):
    seq_count, length_rows, _ = query_key_value.shape
    query_width = query_heads * HEAD_SIZE
    key_width = key_value_heads * HEAD_SIZE
    query_rows = (
        query_key_value[..., :query_width]
        .reshape(seq_count, length_rows, query_heads, HEAD_SIZE)
        .transpose(0, 2, 1, 3)
    )
    key_rows = (
        query_key_value[..., query_width : query_width + key_width]
        .reshape(seq_count, length_rows, key_value_heads, HEAD_SIZE)
        .transpose(0, 2, 1, 3)
    )
    value_rows = (
        query_key_value[..., query_width + key_width :]
        .reshape(seq_count, length_rows, key_value_heads, HEAD_SIZE)
        .transpose(0, 2, 1, 3)
        .astype(jnp.bfloat16)
    )
    query_rows = (
        apply_rotary(query_rows, length_rows)
        .astype(jnp.bfloat16)
        .reshape(seq_count, key_value_heads, query_heads // key_value_heads, length_rows, HEAD_SIZE)
    )
    key_rows = apply_rotary(key_rows, length_rows).astype(jnp.bfloat16)
    scores = jnp.einsum(
        "bgqtd,bgsd->bgqts", query_rows, key_rows, preferred_element_type=jnp.float32
    ) / jnp.sqrt(jnp.float32(HEAD_SIZE))
    places = jnp.arange(length_rows, dtype=jnp.int32)
    causal = places[None, :] <= places[:, None]
    usable = places[None, :] < group_lengths[:, None]
    allowed = causal[None, :, :] & usable[:, None, :]
    scores = jnp.where(allowed[:, None, None, :, :], scores, jnp.float32(-1e30))
    highest = jnp.max(scores, axis=-1, keepdims=True)
    expd = jnp.exp(scores - highest)
    probs = (expd / jnp.sum(expd, axis=-1, keepdims=True)).astype(jnp.bfloat16)
    mixed = jnp.einsum("bgqts,bgsd->bgqtd", probs, value_rows, preferred_element_type=jnp.float32)
    mixed = mixed.reshape(seq_count, query_heads, length_rows, HEAD_SIZE).transpose(0, 2, 1, 3)
    return mixed.reshape(seq_count * length_rows, query_width).astype(jnp.bfloat16)


UP, DOWN, ACROSS = 0, 1, 2


def rotary_tables(length_rows):
    half = HEAD_SIZE // 2
    freqs = 1000000.0 ** (-2.0 * np.arange(half) / HEAD_SIZE)
    angles = np.arange(length_rows)[:, None] * freqs[None, :]
    cosine, sine = np.cos(angles), np.sin(angles)
    return (
        np.concatenate([cosine, cosine], axis=1).astype(np.float32),
        np.concatenate([-sine, sine], axis=1).astype(np.float32),
    )


def layer_kernel(
    shards,
    groups,
    tokens,
    qkv_weight,
    out_weight,
    length,
    pair_weight,
    partner,
    norm_gain_flat,
    final_gain_flat,
    value_head_flat,
    qkv_bias_flat,
    cosine,
    sine,
    hidden,
    margin_out,
    loss_out,
    qkv_full,
    out_full,
    tok_all,
    len_tile,
    len_all,
    normed,
    qkv_rows,
    attn,
    own,
    part_out,
    part_in,
    score_tile,
    score_all,
    partner_rows,
    norm_gain,
    final_gain,
    value_head,
    qkv_bias,
    local_sem,
    recv_sem,
    send_sem,
    tok_send,
    tok_recv,
    len_send,
    len_recv,
    part_send,
    part_recv,
    score_send,
    score_recv,
):
    line = shards // 2
    f = lax.axis_index("fsdp")
    g = lax.axis_index("dp")
    z = f // 2
    y = f % 2
    even = z % 2 == 0
    seq_rows = tokens.shape[0]
    depth = qkv_weight.shape[0]
    width = tok_all.shape[2]
    query_cols = QUERY_FEATURES // groups
    key_cols = KEY_FEATURES // groups
    heads = query_cols // HEAD_SIZE
    half_depth = depth // 2
    half_out = out_weight.shape[0] // 2
    has_up = z < line - 1
    has_down = z > 0

    def slot(m, c, s):
        if m == 0:
            return qkv_full.at[pl.ds(pl.multiple_of(s * depth + c * half_depth, 32), half_depth)]
        return out_full.at[s, pl.ds(c * half_out, half_out)]

    locals_ = [[[], []], [[], []]]
    count = 0
    for c in range(2):
        rows = pl.ds(c * half_depth, half_depth)
        there = slot(0, c, f)
        for start, size, to in (
            (g * query_cols, query_cols, 0),
            (QUERY_FEATURES + g * key_cols, key_cols, query_cols),
            (QUERY_FEATURES + KEY_FEATURES + g * key_cols, key_cols, query_cols + key_cols),
        ):
            locals_[0][c].append(
                pltpu.make_async_copy(
                    qkv_weight.at[rows, pl.ds(pl.multiple_of(start, 128), size)],
                    there.at[:, pl.ds(to, size)],
                    local_sem.at[count],
                )
            )
            count += 1
    for c in range(2):
        locals_[1][c].append(
            pltpu.make_async_copy(
                out_weight.at[
                    pl.ds(c * half_out, half_out),
                    pl.ds(pl.multiple_of(g * query_cols, 128), query_cols),
                ],
                slot(1, c, f),
                local_sem.at[count],
            )
        )
        count += 1
    tok_local = pltpu.make_async_copy(tokens, tok_all.at[g], local_sem.at[count])
    len_tile[...] = jnp.full(len_tile.shape, length[0], jnp.int32)
    len_all[g] = len_tile[...]
    for m in range(2):
        for c in range(2):
            for copy in locals_[m][c]:
                copy.start()
    tok_local.start()
    vectors = [
        pltpu.make_async_copy(flat, row.at[0], local_sem.at[count + 1 + i])
        for i, (flat, row) in enumerate(
            (
                (norm_gain_flat, norm_gain),
                (final_gain_flat, final_gain),
                (value_head_flat, value_head),
                (qkv_bias_flat, qkv_bias),
            )
        )
    ]
    for copy in vectors:
        copy.start()

    barrier = pltpu.get_barrier_semaphore()
    across = 2 * z + 1 - y
    everyone = shards * groups
    me = f * groups + g

    @pl.loop(1, everyone)
    def _(i):
        other = lax.rem(me + i, everyone)
        pl.semaphore_signal(
            barrier, inc=1, device_id={"fsdp": other // groups, "dp": lax.rem(other, groups)}
        )

    peers = [lax.rem(g + i, groups) for i in range(1, groups)]
    pl.semaphore_wait(barrier, everyone - 1)

    started = []

    def send(cond, way, m, c, s):
        target = (f + 2, f - 2, across)[way]
        copy = pltpu.make_async_remote_copy(
            src_ref=slot(m, c, s),
            dst_ref=slot(m, c, s),
            send_sem=send_sem.at[way, m, c, s],
            recv_sem=recv_sem.at[m, c, s],
            device_id={"fsdp": target},
        )
        started.append((cond, copy))
        if cond is None:
            copy.start()
        else:
            pl.when(cond)(copy.start)

    def arrived(m, c, s):
        pltpu.make_async_copy(slot(m, c, s), slot(m, c, s), recv_sem.at[m, c, s]).wait()

    def own_line(m, c):
        send(has_up, UP, m, c, f)
        send(has_down, DOWN, m, c, f)

    def line_step(m, k):
        for c in range(2):
            below = z - k
            above = z + k
            s_below = 2 * jnp.maximum(below, 0) + y
            s_above = 2 * jnp.minimum(above, line - 1) + y

            @pl.when(below >= 0)
            def _():
                arrived(m, c, s_below)

            send((below >= 0) & has_up, UP, m, c, s_below)
            if k > 1 or c == 0:
                send(below >= 0, ACROSS, m, c, s_below)
            else:
                send((below >= 0) & even, ACROSS, m, c, s_below)

            @pl.when(above < line)
            def _():
                arrived(m, c, s_above)

            send((above < line) & has_down, DOWN, m, c, s_above)
            if k > 1 or c == 0:
                send(above < line, ACROSS, m, c, s_above)
            else:
                send((above < line) & jnp.logical_not(even), ACROSS, m, c, s_above)

    def half_step(m):
        arrived(m, 1, across)
        send(even, UP, m, 1, across)
        send(jnp.logical_not(even), DOWN, m, 1, across)

    for c in range(2):
        for copy in locals_[0][c]:
            copy.wait()
        own_line(0, c)
        send(None, ACROSS, 0, c, f)
    small = []
    for peer in peers:
        for source, dest, ss, rs in (
            (tokens, tok_all, tok_send, tok_recv),
            (len_tile, len_all, len_send, len_recv),
        ):
            copy = pltpu.make_async_remote_copy(
                src_ref=source,
                dst_ref=dest.at[g],
                send_sem=ss.at[peer],
                recv_sem=rs.at[g],
                device_id={"dp": peer},
            )
            copy.start()
            small.append(copy)

    line_step(0, 1)
    for k in range(2, line - 1):
        line_step(0, k)
    half_step(0)
    for c in range(2):
        for copy in locals_[1][c]:
            copy.wait()
        own_line(1, c)

    tok_local.wait()
    for copy in vectors:
        copy.wait()
    for peer in peers:
        pltpu.make_async_copy(tok_all.at[peer], tok_all.at[peer], tok_recv.at[peer]).wait()
        pltpu.make_async_copy(len_all.at[peer], len_all.at[peer], len_recv.at[peer]).wait()

    norm_rows = 16
    for j in range(groups):

        @pl.loop(0, seq_rows // norm_rows)
        def _(i):
            at = pl.multiple_of(i * norm_rows, norm_rows)
            rows = tok_all[j, pl.ds(at, norm_rows), :].astype(jnp.float32)
            scale = lax.rsqrt(jnp.mean(rows * rows, axis=-1, keepdims=True) + 1e-06)
            normed[pl.ds(pl.multiple_of(j * seq_rows + at, norm_rows), norm_rows), :] = (
                rows * scale * norm_gain[...]
            ).astype(jnp.bfloat16)

    line_step(0, line - 1)
    for c in range(2):
        send(None, ACROSS, 1, c, f)

    def across_wait(m, k):
        for c in range(2):
            if k == 0:
                if c == 0:
                    arrived(m, c, across)
                continue
            for there, ok in ((z - k, z - k >= 0), (z + k, z + k < line)):
                s = 2 * jnp.clip(there, 0, line - 1) + 1 - y

                @pl.when(ok)
                def _():
                    arrived(m, c, s)

    for k in range(line):
        across_wait(0, k)

    tile = 3 * HEAD_SIZE

    @pl.loop(0, (query_cols + 2 * key_cols) // tile)
    def _(t):
        cols = pl.ds(pl.multiple_of(t * tile, tile), tile)
        qkv_rows[:, cols] = jnp.dot(
            normed[...], qkv_full[:, cols], preferred_element_type=jnp.float32
        )

    def head_rows(j, column, bias_at):
        rows = qkv_rows[pl.ds(pl.multiple_of(j * seq_rows, seq_rows), seq_rows), pl.ds(column, HEAD_SIZE)]
        return rows + qkv_bias[:, pl.ds(pl.multiple_of(bias_at, HEAD_SIZE), HEAD_SIZE)]

    def rotate(rows):
        return (
            rows * cosine[...] + pltpu.roll(rows, HEAD_SIZE // 2, 1) * sine[...]
        ).astype(jnp.bfloat16)

    key_heads = key_cols // HEAD_SIZE
    share = heads // key_heads

    def attend_sequence(j):
        query_place = lax.broadcasted_iota(jnp.int32, (seq_rows, seq_rows), 0)
        key_place = lax.broadcasted_iota(jnp.int32, (seq_rows, seq_rows), 1)
        allowed = (key_place <= query_place) & (key_place < len_all[j, 0:1, :])
        at = pl.ds(pl.multiple_of(j * seq_rows, seq_rows), seq_rows)
        for kh in range(key_heads):
            offset = kh * HEAD_SIZE
            key = rotate(
                head_rows(j, query_cols + offset, QUERY_FEATURES + g * key_cols + offset)
            )
            value = head_rows(
                j,
                query_cols + key_cols + offset,
                QUERY_FEATURES + KEY_FEATURES + g * key_cols + offset,
            ).astype(jnp.bfloat16)
            for h in range(kh * share, (kh + 1) * share):
                query = rotate(head_rows(j, h * HEAD_SIZE, g * query_cols + h * HEAD_SIZE))
                scores = lax.dot_general(
                    query, key, (((1,), (1,)), ((), ())), preferred_element_type=jnp.float32
                ) / np.float32(np.sqrt(HEAD_SIZE))
                scores = jnp.where(allowed, scores, jnp.float32(-1e30))
                expd = jnp.exp(scores - jnp.max(scores, axis=-1, keepdims=True))
                probs = (expd / jnp.sum(expd, axis=-1, keepdims=True)).astype(jnp.bfloat16)
                attn[at, h * HEAD_SIZE : (h + 1) * HEAD_SIZE] = jnp.dot(
                    probs, value, preferred_element_type=jnp.float32
                ).astype(jnp.bfloat16)

    pl.loop(0, groups // 2)(attend_sequence)
    line_step(1, 1)
    pl.loop(groups // 2, groups)(attend_sequence)

    def part_copy(peer, s):
        return pltpu.make_async_remote_copy(
            src_ref=part_out.at[s, pl.ds(pl.multiple_of(peer * seq_rows, seq_rows), seq_rows)],
            dst_ref=part_in.at[g, s],
            send_sem=part_send.at[peer, s],
            recv_sem=part_recv.at[g, s],
            device_id={"dp": peer},
        )

    def project(s):
        result = lax.dot_general(
            attn[...],
            out_full[s],
            (((1,), (1,)), ((), ())),
            preferred_element_type=jnp.float32,
        )
        part_out[s] = result.astype(jnp.bfloat16)
        for j in range(groups):

            @pl.when(g == j)
            def _():
                own[s] = result[j * seq_rows : (j + 1) * seq_rows]

        for peer in peers:
            part_copy(peer, s).start()

    def project_places(k, side):
        @pl.loop(0, 1 if k == 0 else 2)
        def _(i):
            there = z + (2 * i - 1) * k

            @pl.when((there >= 0) & (there < line))
            def _():
                project(2 * there + side)

    for k in range(2, line - 1):
        line_step(1, k)
    half_step(1)
    across_wait(1, 0)

    @pl.loop(0, 2)
    def _(side):
        project(2 * z + side)

    project_places(1, y)
    line_step(1, line - 1)
    for k in range(2, line):
        project_places(k, y)
    for k in range(1, line):
        across_wait(1, k)
        project_places(k, 1 - y)

    @pl.loop(0, shards)
    def _(s):
        for peer in peers:
            pltpu.make_async_copy(
                part_in.at[peer, s], part_in.at[peer, s], part_recv.at[peer, s]
            ).wait()

    block = 32
    out_cols = own.shape[2]

    @pl.loop(0, seq_rows // block)
    def _(i):
        at = pl.ds(pl.multiple_of(i * block, block), block)
        for p in range(shards // 2):
            sums = []
            for s in (2 * p, 2 * p + 1):
                total = own[s, at]
                for peer in peers:
                    total += part_in[peer, s, at].astype(jnp.float32)
                sums.append(total)
            cols = slice(2 * p * out_cols, 2 * (p + 1) * out_cols)
            hidden[at, cols] = (
                tok_all[g, at, cols].astype(jnp.float32) + jnp.concatenate(sums, axis=1)
            ).astype(jnp.bfloat16)

    place = lax.broadcasted_iota(jnp.int32, len_tile.shape, 1)
    pick = (place == len_tile[...] - 1).astype(jnp.bfloat16)
    last = jnp.dot(pick, hidden[...], preferred_element_type=jnp.float32)
    scale = lax.rsqrt(jnp.mean(last * last, axis=-1, keepdims=True) + 1e-06)
    score = jnp.sum(last * scale * final_gain[...] * value_head[...], axis=-1, keepdims=True)
    first_row = lax.broadcasted_iota(jnp.int32, score_tile.shape, 0) == 0
    score_tile[...] = jnp.where(first_row, score, jnp.full(score_tile.shape, pair_weight[0]))
    score_all[me] = score_tile[...]

    def score_copy(i):
        other = lax.rem(me + i, everyone)
        return pltpu.make_async_remote_copy(
            src_ref=score_tile,
            dst_ref=score_all.at[me],
            send_sem=score_send.at[other],
            recv_sem=score_recv.at[me],
            device_id={"fsdp": other // groups, "dp": lax.rem(other, groups)},
        )

    @pl.loop(1, everyone)
    def _(i):
        score_copy(i).start()

    @pl.loop(0, everyone)
    def _(i):
        partner_rows[pl.ds(i, 1), :] = jnp.full((1, HEAD_SIZE), partner[i], jnp.int32)

    @pl.loop(1, everyone)
    def _(i):
        other = lax.rem(me + i, everyone)
        pltpu.make_async_copy(
            score_all.at[other], score_all.at[other], score_recv.at[other]
        ).wait()

    scores = score_all[:, 0, :]
    weights = score_all[:, 1, :]
    row = lax.broadcasted_iota(jnp.int32, scores.shape, 0)
    lane = lax.broadcasted_iota(jnp.int32, scores.shape, 1)
    partners = partner_rows[...]
    score_row = jnp.sum(jnp.where(row == lane, scores, 0.0), axis=0, keepdims=True)
    others = jnp.sum(jnp.where(partners == lane, score_row, 0.0), axis=1, keepdims=True)
    margins = jnp.where(row < partners, scores - others, others - scores)
    softplus = jnp.maximum(-margins, 0.0) + jnp.log1p(jnp.exp(-jnp.abs(margins)))
    first_lane = lane == 0
    margin_out[0] = jnp.sum(jnp.where(first_lane & (row == me), margins, 0.0))
    loss_out[0] = jnp.sum(jnp.where(first_lane, weights * softplus, 0.0)) / everyone

    for cond, copy in started:
        if cond is None:
            copy.wait_send()
        else:
            pl.when(cond)(copy.wait_send)
    for copy in small:
        copy.wait_send()

    @pl.loop(0, shards)
    def _(s):
        for peer in peers:
            part_copy(peer, s).wait_send()

    @pl.loop(1, everyone)
    def _(i):
        score_copy(i).wait_send()


def layer_fits(shards, groups, tokens, qkv_weight, out_weight):
    return (
        shards % 4 == 0
        and shards >= 8
        and qkv_weight.shape[0] % 32 == 0
        and KEY_VALUE_HEADS % groups == 0
        and tokens.shape[1] == HEAD_SIZE
        and groups % 2 == 0
        and shards * groups <= HEAD_SIZE
        and out_weight.shape[1] % 64 == 0
    )


def layer(
    tokens,
    lengths,
    partner,
    pair_weight,
    norm_gain,
    qkv_weight,
    qkv_bias,
    out_weight,
    final_gain,
    value_head,
):
    shards, groups = lax.axis_size("fsdp"), lax.axis_size("dp")
    _, seq_rows, width = tokens.shape
    depth = qkv_weight.shape[0]
    out_cols = out_weight.shape[1]
    query_cols = QUERY_FEATURES // groups
    key_cols = KEY_FEATURES // groups
    all_cols = query_cols + 2 * key_cols
    rows = groups * seq_rows
    cosine, sine = rotary_tables(seq_rows)
    everyone = shards * groups
    dma = pltpu.SemaphoreType.DMA
    vmem = pl.BlockSpec(memory_space=pltpu.VMEM)
    anywhere = pl.BlockSpec(memory_space=pl.ANY)
    bf16, f32 = jnp.bfloat16, jnp.float32
    scalar = pl.BlockSpec(memory_space=pltpu.SMEM)
    hidden, margin, loss = pl.pallas_call(
        functools.partial(layer_kernel, shards, groups),
        out_shape=(
            jax.ShapeDtypeStruct((seq_rows, width), bf16),
            jax.ShapeDtypeStruct((1,), f32),
            jax.ShapeDtypeStruct((1,), f32),
        ),
        in_specs=[anywhere] * 3 + [scalar] * 3 + [anywhere] * 4 + [vmem] * 2,
        out_specs=(vmem, scalar, scalar),
        scratch_shapes=[
            pltpu.VMEM((shards * depth, all_cols), bf16),
            pltpu.VMEM((shards, out_cols, query_cols), bf16),
            pltpu.VMEM((groups, seq_rows, width), bf16),
            pltpu.VMEM((8, seq_rows), jnp.int32),
            pltpu.VMEM((groups, 8, seq_rows), jnp.int32),
            pltpu.VMEM((rows, width), bf16),
            pltpu.VMEM((rows, all_cols), f32),
            pltpu.VMEM((rows, query_cols), bf16),
            pltpu.VMEM((shards, seq_rows, out_cols), f32),
            pltpu.VMEM((shards, rows, out_cols), bf16),
            pltpu.VMEM((groups, shards, seq_rows, out_cols), bf16),
            pltpu.VMEM((8, HEAD_SIZE), f32),
            pltpu.VMEM((everyone, 8, HEAD_SIZE), f32),
            pltpu.VMEM((everyone, HEAD_SIZE), jnp.int32),
            pltpu.VMEM((1, width), f32),
            pltpu.VMEM((1, width), f32),
            pltpu.VMEM((1, width), f32),
            pltpu.VMEM((1, qkv_bias.shape[0]), f32),
            dma((13,)),
            dma((2, 2, shards)),
            dma((3, 2, 2, shards)),
            dma((groups,)),
            dma((groups,)),
            dma((groups,)),
            dma((groups,)),
            dma((groups, shards)),
            dma((groups, shards)),
            dma((everyone,)),
            dma((everyone,)),
        ],
        compiler_params=pltpu.CompilerParams(
            collective_id=0, has_side_effects=True, vmem_limit_bytes=60 * 1024 * 1024
        ),
    )(
        tokens[0],
        qkv_weight,
        out_weight.T,
        lengths,
        pair_weight,
        partner,
        norm_gain,
        final_gain,
        value_head,
        qkv_bias,
        jnp.asarray(cosine),
        jnp.asarray(sine),
    )
    return hidden[None], margin, loss.reshape(())


def projected_by_gathers(
    tokens,
    lengths,
    norm_gain,
    qkv_weight,
    qkv_bias,
    out_weight,
):
    sequence = tokens[0]
    length_rows = sequence.shape[0]
    width = sequence.shape[1]
    normed = rms_scale(sequence.astype(jnp.float32), norm_gain).astype(jnp.bfloat16)
    query_group_count = lax.axis_size("dp")
    group_index = lax.axis_index("dp")
    query_heads = QUERY_HEADS // query_group_count
    key_value_heads = KEY_VALUE_HEADS // query_group_count
    query_cols = query_heads * HEAD_SIZE
    key_cols = key_value_heads * HEAD_SIZE
    group_normed, group_lengths = (
        lax.all_gather(normed[None], "dp", axis=0, tiled=True),
        lax.all_gather(lengths, "dp", axis=0, tiled=True),
    )
    seq_count = group_normed.shape[0]
    flat = group_normed.reshape(seq_count * length_rows, width)
    qkv_cols = jnp.concatenate(
        [
            lax.dynamic_slice_in_dim(qkv_weight, group_index * query_cols, query_cols, 1),
            lax.dynamic_slice_in_dim(
                qkv_weight, QUERY_FEATURES + group_index * key_cols, key_cols, 1
            ),
            lax.dynamic_slice_in_dim(
                qkv_weight, QUERY_FEATURES + KEY_FEATURES + group_index * key_cols, key_cols, 1
            ),
        ],
        axis=1,
    )
    bias_cols = jnp.concatenate(
        [
            lax.dynamic_slice_in_dim(qkv_bias, group_index * query_cols, query_cols, 0),
            lax.dynamic_slice_in_dim(
                qkv_bias, QUERY_FEATURES + group_index * key_cols, key_cols, 0
            ),
            lax.dynamic_slice_in_dim(
                qkv_bias, QUERY_FEATURES + KEY_FEATURES + group_index * key_cols, key_cols, 0
            ),
        ],
        axis=0,
    )
    out_rows = lax.dynamic_slice_in_dim(out_weight, group_index * query_cols, query_cols, 0)
    qkv_full, out_full = (
        lax.all_gather(qkv_cols, "fsdp", axis=0, tiled=True),
        lax.all_gather(out_rows, "fsdp", axis=1, tiled=True),
    )
    query_key_value = jnp.dot(flat, qkv_full, preferred_element_type=jnp.float32) + bias_cols
    attn = attend(
        query_key_value.reshape(seq_count, length_rows, -1),
        group_lengths,
        query_heads,
        key_value_heads,
    )
    return lax.psum_scatter(
        jnp.dot(attn, out_full, preferred_element_type=jnp.float32),
        "dp",
        scatter_dimension=0,
        tiled=True,
    )


def per_device(
    tokens,
    lengths,
    partner,
    pair_weight,
    norm_gain,
    qkv_weight,
    qkv_bias,
    out_weight,
    final_gain,
    value_head,
):
    if layer_fits(lax.axis_size("fsdp"), lax.axis_size("dp"), tokens, qkv_weight, out_weight):
        return layer(
            tokens,
            lengths,
            partner,
            pair_weight,
            norm_gain,
            qkv_weight,
            qkv_bias,
            out_weight,
            final_gain,
            value_head,
        )
    sequence = tokens[0]
    length = lengths[0]
    projected = projected_by_gathers(tokens, lengths, norm_gain, qkv_weight, qkv_bias, out_weight)
    hidden = (sequence.astype(jnp.float32) + projected).astype(jnp.bfloat16)
    last = lax.dynamic_slice_in_dim(hidden, length - 1, 1, 0)[0].astype(jnp.float32)
    score = jnp.sum(rms_scale(last, final_gain) * value_head)
    everyone, weights_all = (
        lax.all_gather(score.reshape(1), ("fsdp", "dp"), axis=0, tiled=True),
        lax.all_gather(pair_weight, ("fsdp", "dp"), axis=0, tiled=True),
    )
    total_seqs = everyone.shape[0]
    mine = lax.axis_index(("fsdp", "dp"))
    index_all = jnp.arange(total_seqs, dtype=jnp.int32)
    my_partner = jnp.sum(jnp.where(index_all == mine, partner, 0))
    other = jnp.sum(jnp.where(index_all == my_partner, everyone, jnp.float32(0.0)))
    margin = jnp.where(mine < my_partner, score - other, other - score)
    matches = partner[:, None] == index_all[None, :]
    others_all = jnp.sum(jnp.where(matches, everyone[None, :], jnp.float32(0.0)), axis=1)
    margins_all = jnp.where(index_all < partner, everyone - others_all, others_all - everyone)
    loss = jnp.sum(weights_all * jax.nn.softplus(-margins_all)) / total_seqs
    return (hidden[None], margin.reshape(1), loss)


def solution(mesh):
    return jax.shard_map(
        per_device,
        mesh=mesh,
        in_specs=(
            P(("fsdp", "dp"), None, None),
            P(("fsdp", "dp")),
            P(),
            P(("fsdp", "dp")),
            P(),
            P("fsdp", None),
            P(),
            P(None, "fsdp"),
            P(),
            P(),
        ),
        out_specs=(P(("fsdp", "dp"), None, None), P(("fsdp", "dp")), P()),
        check_vma=False,
    )
```
